32 devices in a mesh: dp: 8 (over y, x, core), space: 4 (over z).
Axes of the slice: x: 2, y: 2, z: 4, core: 2. Of those that a mesh axis runs over, the one named last changes fastest.
Arguments:
- act_in: bfloat16 [8, 8, 64, 2048], P('dp', 'space'), may hold values from -6 to 6
- weight_one: bfloat16 [3, 3, 3, 32, 64], replicated, may hold values from -0.21875 to 0.21875
- bias_one: float32 [64], replicated, may hold values from -3 to 3
- weight_two: bfloat16 [3, 3, 3, 64, 128], replicated, may hold values from -0.15625 to 0.15625
- bias_two: float32 [128], replicated, may hold values from -3 to 3
- cotangent: bfloat16 [8, 4, 32, 4096], P('dp', 'space'), may hold values from -24 to 24
Outputs:
- grad_input: bfloat16 [8, 8, 64, 2048], P('dp', 'space')
- grad_w_one: float32 [3, 3, 3, 32, 64], replicated
- grad_b_one: float32 [64], replicated
- grad_w_two: float32 [3, 3, 3, 64, 128], replicated
- grad_b_two: float32 [128], replicated
The draws below stay inside these ranges and needn't reach their ends.
All inputs are finite; a program needn't handle non-finite values.
Results may differ from the reference program's by a relative error of at most 0.01.
Values may be sent and summed in bfloat16 or wider, within the bound.
A program may use at most 128 MiB of HBM per device.

```python
import math
import jax
import jax.numpy as jnp
from jax import lax

C0 = 32
C1 = 64
C2 = 128
SIDE = 64
BATCH = 8
DEPTH = 8
DEPTH2 = 4
HALF = 32


def levels(rng, shape, shards, smallest, high):
    gain = 1.0
    for dim, blocks in shards:
        draws = jax.random.uniform(jax.random.fold_in(jax.random.fold_in(rng, 6), dim), (blocks,), jnp.float32, smallest / len(shards), high / len(shards))
        gain = gain * jnp.repeat(jnp.exp(draws), shape[dim] // blocks).reshape((-1,) + (1,) * (len(shape) - 1 - dim))
    return gain


def centred(stream_key, dims, deviation, reach, cuts=(), kind=jnp.bfloat16):
    gain = levels(stream_key, dims, cuts, -0.22, 0.18) if cuts else 1.0
    drawn = jax.random.normal(stream_key, dims, jnp.float32) * deviation * gain
    return jnp.minimum(jnp.maximum(drawn, -reach), reach).astype(kind)


def setup_inputs(seed: int = 0) -> dict:
    splits = jax.random.split(jax.random.key(seed), 7)
    return {
        "act_in": centred(splits[0], (BATCH, DEPTH, SIDE, SIDE * C0), 1.0, 6.0, ((0, 8), (1, 4))),
        "weight_one": centred(splits[1], (3, 3, 3, C0, C1), (27 * C0) ** -0.5, 0.21875),
        "bias_one": centred(splits[2], (C1,), 0.5, 3.0, (), jnp.float32),
        "weight_two": centred(splits[3], (3, 3, 3, C1, C2), (27 * C1) ** -0.5, 0.15625),
        "bias_two": centred(splits[4], (C2,), 0.5, 3.0, (), jnp.float32),
        "cotangent": centred(splits[5], (BATCH, DEPTH2, HALF, HALF * C2), 4.0, 24.0, ((0, 8), (1, 4))),
    }


def forward_conv(padded, kernel):
    return lax.conv_general_dilated(padded, kernel, (1, 1, 1), ((0, 0), (1, 1), (1, 1)), dimension_numbers=('NDHWC', 'DHWIO', 'NDHWC'), preferred_element_type=jnp.float32)

def weight_grad(padded, delta):
    return lax.conv_general_dilated(padded, delta, (1, 1, 1), ((0, 0), (1, 1), (1, 1)), dimension_numbers=('CDHWN', 'IDHWO', 'DHWNC'), preferred_element_type=jnp.float32)

def input_grad(delta, kernel, depth_pad):
    return lax.conv_general_dilated(delta, kernel[::-1, ::-1, ::-1], (1, 1, 1), (depth_pad, (1, 1), (1, 1)), dimension_numbers=('NDHWC', 'DHWOI', 'NDHWC'), preferred_element_type=jnp.float32)

def silu_slope(value):
    sig = jax.nn.sigmoid(value)
    return sig * (1.0 + value * (1.0 - sig))

def reference(act_in, weight_one, bias_one, weight_two, bias_two, cotangent):

    def single(pair):
        sample, cot = pair
        x_five = sample.reshape(1, DEPTH, SIDE, SIDE, C0)
        x_pad = jnp.pad(x_five, ((0, 0), (1, 1), (0, 0), (0, 0), (0, 0)))
        pre_one = forward_conv(x_pad, weight_one) + bias_one
        act_one = pre_one * jax.nn.sigmoid(pre_one)
        pooled = act_one.reshape(1, DEPTH2, 2, HALF, 2, HALF, 2, C1).mean(axis=(2, 4, 6)).astype(jnp.bfloat16)
        pool_pad = jnp.pad(pooled, ((0, 0), (1, 1), (0, 0), (0, 0), (0, 0)))
        pre_two = forward_conv(pool_pad, weight_two) + bias_two
        cot_five = cot.reshape(1, DEPTH2, HALF, HALF, C2).astype(jnp.float32)
        delta_two = (cot_five * silu_slope(pre_two)).astype(jnp.bfloat16)
        gw_two = weight_grad(pool_pad, delta_two)
        gb_two = lax.optimization_barrier(jnp.sum(delta_two, axis=(0, 1, 2, 3), dtype=jnp.float32))
        grad_pooled = input_grad(delta_two, weight_two, (1, 1))
        spread = jnp.broadcast_to(grad_pooled[:, :, None, :, None, :, None, :], (1, DEPTH2, 2, HALF, 2, HALF, 2, C1)).reshape(1, DEPTH, SIDE, SIDE, C1)
        delta_one = (spread / 8.0 * silu_slope(pre_one)).astype(jnp.bfloat16)
        gw_one = weight_grad(x_pad, delta_one)
        gb_one = lax.optimization_barrier(jnp.sum(delta_one, axis=(0, 1, 2, 3), dtype=jnp.float32))
        grad_x = input_grad(delta_one, weight_one, (1, 1)).astype(jnp.bfloat16).reshape(DEPTH, SIDE, SIDE * C0)
        return (grad_x, gw_one, gb_one, gw_two, gb_two)
    grad_x, gw_one, gb_one, gw_two, gb_two = lax.map(single, (act_in, cotangent))
    scale_one = 16.0 / math.sqrt(BATCH * DEPTH * SIDE * SIDE)
    scale_two = 1.0 / math.sqrt(BATCH * DEPTH2 * HALF * HALF)
    return (grad_x, lax.optimization_barrier(jnp.sum(gw_one, axis=0)) * scale_one, lax.optimization_barrier(jnp.sum(gb_one, axis=0)) * scale_one, lax.optimization_barrier(jnp.sum(gw_two, axis=0)) * scale_two, lax.optimization_barrier(jnp.sum(gb_two, axis=0)) * scale_two)
```

```python
import functools
import math

import jax
import jax.numpy as jnp
from jax import lax
from jax.experimental import pallas as pl
from jax.experimental.pallas import tpu as pltpu
from jax.sharding import PartitionSpec as P

MESH = pl.DeviceIdType.MESH
F32 = jnp.float32
BF16 = jnp.bfloat16


def dot(a, b):
    return lax.dot_general(a, b, (((1,), (0,)), ((), ())), preferred_element_type=F32)


def dot_t(a, b):
    return lax.dot_general(a, b, (((1,), (1,)), ((), ())), preferred_element_type=F32)


def sigmoid(x):
    return 0.5 * jnp.tanh(0.5 * x) + 0.5


def slope(x):
    s = sigmoid(x)
    return s * (1.0 + x * (1.0 - s))


def lanes(shape):
    return lax.broadcasted_iota(jnp.int32, shape, 1)


def from_left(x, wide):
    g = lax.broadcasted_iota(jnp.int32, x.shape, 0) % wide
    return jnp.where(g == 0, 0.0, pltpu.roll(x, 1, 0))


def from_right(x, wide):
    g = lax.broadcasted_iota(jnp.int32, x.shape, 0) % wide
    return jnp.where(g == wide - 1, 0.0, pltpu.roll(x, x.shape[0] - 1, 0))


def edge_lanes(x, wide):
    return jnp.where(lanes(x.shape) < 64, from_right(x, wide), from_left(x, wide))


class Sum:
    def __init__(self, n, m, me, my, each, x, got, part, gots, out, acc, sems):
        self.n, self.m, self.me, self.my, self.each = n, m, me, my, each
        self.x, self.got, self.part, self.gots, self.out, self.acc = x, got, part, gots, out, acc
        self.send, self.recv, self.send_s, self.recv_s = sems

    def rows(self, count, start):
        return pl.ds(pl.multiple_of(start * self.each, 16), count * self.each)

    def to_dp(self, k, src, dst, base):
        return pltpu.make_async_remote_copy(
            src_ref=src,
            dst_ref=dst,
            send_sem=self.send.at[base + k],
            recv_sem=self.recv.at[base + k],
            device_id=(lax.rem(self.me + k, self.n), self.my),
            device_id_type=MESH,
        )

    def to_space(self, k, src, dst, base):
        return pltpu.make_async_remote_copy(
            src_ref=src,
            dst_ref=dst,
            send_sem=self.send_s.at[base + k],
            recv_sem=self.recv_s.at[base + k],
            device_id=(self.me, lax.rem(self.my + k, self.m)),
            device_id_type=MESH,
        )

    def step1(self):
        n, m = self.n, self.m
        self.c1 = []
        for k in range(1, n):
            src = self.x.at[self.rows(m, lax.rem(self.me + k, n) * m)]
            self.c1.append(self.to_dp(k, src, self.got.at[k], 0))
        for c in self.c1:
            c.start()

    def step2(self):
        n, m, each = self.n, self.m, self.each
        for c in self.c1:
            c.wait_recv()
        total = self.x[self.rows(m, self.me * m), :].astype(F32)
        for k in range(1, n):
            total = total + self.got[k].astype(F32)
        self.acc[...] = total
        self.part[...] = total.astype(BF16)
        self.c2 = []
        for k in range(1, m):
            src = self.part.at[self.rows(1, lax.rem(self.my + k, m))]
            self.c2.append(self.to_space(k, src, self.gots.at[k], 0))
        for c in self.c2:
            c.start()
        for c in self.c1:
            c.wait_send()

    def step3(self):
        m = self.m
        for c in self.c2:
            c.wait_recv()
        total = self.acc[self.rows(1, self.my), :]
        for k in range(1, m):
            total = total + self.gots[k].astype(F32)
        mine = self.rows(1, self.me * m + self.my)
        self.out[mine, :] = total.astype(BF16)
        self.c3 = [self.to_space(k, self.out.at[mine], self.out.at[mine], m) for k in range(1, m)]
        for c in self.c3:
            c.start()
        for c in self.c2:
            c.wait_send()

    def step4(self):
        n, m = self.n, self.m
        for c in self.c3:
            c.wait_recv()
        mine = self.rows(m, self.me * m)
        self.c4 = [self.to_dp(k, self.out.at[mine], self.out.at[mine], n) for k in range(1, n)]
        for c in self.c4:
            c.start()
        for c in self.c3:
            c.wait_send()

    def step5(self):
        for c in self.c4:
            c.wait_recv()
        for c in self.c4:
            c.wait_send()


def kernel(
    n, m, scale_one, scale_two, each1, each2,
    act, w1, b1, w2, b2, cot,
    gin, gw1, gb1, gw2, gb2,
    xr, x2, pre1, pool, p2, pre2, cotr, d2, d2t, gp, d1, d1t, gx,
    k1, k2, g1, g2, b1s, b2s, gb1s, gb2s, fold1,
    acth, poolh, gps, gpr, gxs, gxr,
    s2x, s2got, s2part, s2gots, s2out, s2acc,
    s1x, s1got, s1part, s1gots, s1out, s1acc,
    hsend, hrecv, dsend2, drecv2, zsend2, zrecv2, dsend1, drecv1, zsend1, zrecv1,
):
    me = lax.axis_index("dp")
    my = lax.axis_index("space")
    slab, side, merged = act.shape[1:]
    wide = merged // 128
    slab2, half = cot.shape[1:3]
    rows, rows2 = side * wide, half * wide
    chan_in, chan_mid = w1.shape[1:]
    chan_out = w2.shape[2]
    big = min(512, rows2)
    small = 256

    barrier = pltpu.get_barrier_semaphore()
    for k in range(1, n):
        pl.semaphore_signal(barrier, inc=1, device_id=(lax.rem(me + k, n), my), device_id_type=MESH)
    for k in range(1, m):
        pl.semaphore_signal(barrier, inc=1, device_id=(me, lax.rem(my + k, m)), device_id_type=MESH)

    def loop(count, body):
        if count == 1:
            body(0)
        else:
            lax.fori_loop(0, count, lambda i, c: (body(i), c)[1], 0)

    def at(i, size, shift=0):
        return pl.ds(pl.multiple_of(i * size + shift, 16), size)

    def down(e, src, dst):
        return pltpu.make_async_remote_copy(
            src_ref=src, dst_ref=dst.at[1], send_sem=hsend.at[2 * e], recv_sem=hrecv.at[2 * e],
            device_id=(me, jnp.maximum(my - 1, 0)), device_id_type=MESH,
        )

    def up(e, src, dst):
        return pltpu.make_async_remote_copy(
            src_ref=src, dst_ref=dst.at[0], send_sem=hsend.at[2 * e + 1], recv_sem=hrecv.at[2 * e + 1],
            device_id=(me, jnp.minimum(my + 1, m - 1)), device_id_type=MESH,
        )

    def send_halo(e, first, last, dst):
        @pl.when(my > 0)
        def _():
            down(e, first, dst).start()

        @pl.when(my < m - 1)
        def _():
            up(e, last, dst).start()

    def wait_halo(e, first, last, dst):
        @pl.when(my > 0)
        def _():
            up(e, last, dst).wait_recv()
            down(e, first, dst).wait_send()

        @pl.when(my < m - 1)
        def _():
            down(e, first, dst).wait_recv()
            up(e, last, dst).wait_send()

        @pl.when(my == 0)
        def _():
            dst[0] = jnp.zeros(dst.shape[1:], dst.dtype)

        @pl.when(my == m - 1)
        def _():
            dst[1] = jnp.zeros(dst.shape[1:], dst.dtype)

    k1[...] = jnp.zeros(k1.shape, BF16)
    for k in range(3):
        for j in range(3):
            for i in range(3):
                tap = w1[(k * 3 + j) * 3 + i]
                for b in range(4):
                    row = ((b + i - 1) * chan_in) % 256 + (k * 3 + j) * 256
                    k1[row : row + chan_in, b * chan_mid : (b + 1) * chan_mid] = tap

    for b in range(4):
        b1s[0:1, b * chan_mid : (b + 1) * chan_mid] = b1[...]
    for b in range(2):
        b2s[0:1, b * chan_out : (b + 1) * chan_out] = b2[...]

    pl.semaphore_wait(barrier, n + m - 2)
    send_halo(0, act.at[0, 0], act.at[0, slab - 1], acth)

    def clear_edges(ref, planes, count):
        for d in range(planes):
            ref[d, 0:wide, :] = jnp.zeros((wide, ref.shape[2]), BF16)
            ref[d, count + wide : count + 2 * wide, :] = jnp.zeros((wide, ref.shape[2]), BF16)

    clear_edges(x2, slab + 2, rows)
    clear_edges(p2, slab2 + 2, rows2)
    clear_edges(d2, slab2, rows2)
    clear_edges(d1, slab, rows)

    def load_plane(src, d):
        for g in range(wide):
            xr[pl.ds(g, side, stride=wide), :] = src[:, g * 128 : (g + 1) * 128].astype(F32)

        def body(r):
            main = xr[at(r, small), :]
            x2[d, at(r, small, wide), 0:128] = main.astype(BF16)
            x2[d, at(r, small, wide), 128:256] = edge_lanes(main, wide).astype(BF16)

        loop(rows // small, body)

    for d in range(slab):
        load_plane(act.at[0, d], d + 1)

    def taps(ref, planes, r, size, shifts):
        return jnp.concatenate([ref[p, at(r, size, s * wide), :] for p in planes for s in shifts], axis=1)

    for d in range(slab):
        ks = [k for k in range(3) if 0 <= d + k - 1 < slab]

        def body(r, d=d, ks=ks):
            left = taps(x2, [d + k for k in ks], r, big, (0, 1, 2))
            pre1[d, at(r, big), :] = dot(left, k1[ks[0] * 768 : (ks[-1] + 1) * 768, :])

        loop(rows // big, body)

    k2[...] = jnp.zeros(k2.shape, BF16)
    for k in range(3):
        for j in range(3):
            for i in range(3):
                tap = w2[(k * 3 + j) * 3 + i]
                for b in range(2):
                    row = ((b + i - 1) * chan_mid) % 256 + (k * 3 + j) * 256
                    k2[row : row + chan_mid, b * chan_out : (b + 1) * chan_out] = tap
    for d in range(slab2):
        for g in range(wide):
            for t in range(2):
                cotr[d, t, pl.ds(g, half, stride=wide), :] = cot[0, d, :, g * 256 + t * 128 : g * 256 + t * 128 + 128].astype(F32)

    wait_halo(0, act.at[0, 0], act.at[0, slab - 1], acth)
    load_plane(acth.at[0], 0)
    load_plane(acth.at[1], slab + 1)

    def put_pooled(d, r, size, main):
        p2[d, at(r, size, wide), 0:128] = main.astype(BF16)
        p2[d, at(r, size, wide), 128:256] = edge_lanes(main, wide).astype(BF16)

    for e in range(slab2):

        def body(r, e=e):
            total = None
            for d in (2 * e, 2 * e + 1):
                pre = pre1[d, at(r, big), :] + b1s[0:1, :]
                if d == 0:
                    pre = pre + dot(taps(x2, [0], r, big, (0, 1, 2)), k1[0:768, :])
                if d == slab - 1:
                    pre = pre + dot(taps(x2, [slab + 1], r, big, (0, 1, 2)), k1[1536:2304, :])
                pre1[d, at(r, big), :] = pre
                one = pre * sigmoid(pre)
                total = one if total is None else total + one
            pairs = total.reshape(big // (2 * wide), 2, wide, 256)
            quad = (pairs[:, 0] + pairs[:, 1]).reshape(big // 2, 256)
            a, b = quad[:, 0:128], quad[:, 128:256]
            a = a + pltpu.roll(a, 64, 1)
            b = b + pltpu.roll(b, 64, 1)
            mean = (jnp.where(lanes(a.shape) < 64, a, b) * 0.125).astype(BF16)
            pool[e, at(r, big // 2), :] = mean
            put_pooled(e + 1, r, big // 2, mean.astype(F32))

        loop(rows // big, body)

    send_halo(1, pool.at[0], pool.at[slab2 - 1], poolh)

    for e in range(slab2):
        ks = [k for k in range(3) if 0 <= e + k - 1 < slab2]

        def body(r, e=e, ks=ks):
            left = taps(p2, [e + k for k in ks], r, big, (0, 1, 2))
            pre2[e, at(r, big), :] = dot(left, k2[ks[0] * 768 : (ks[-1] + 1) * 768, :])

        loop(rows2 // big, body)

    g2[...] = jnp.zeros(g2.shape, BF16)
    g1[...] = jnp.zeros(g1.shape, BF16)
    for k in range(3):
        for j in range(3):
            for i in range(3):
                tap = w2[(k * 3 + j) * 3 + i]
                for b in range(2):
                    lane = j * 512 + ((b - i + 1) * chan_out) % 512
                    g2[k * 128 + b * chan_mid : k * 128 + (b + 1) * chan_mid, lane : lane + chan_out] = tap
                tap = w1[(k * 3 + j) * 3 + i]
                for b in range(4):
                    lane = j * 384 + ((b - i + 1) * chan_mid) % 384
                    g1[k * 128 + b * chan_in : k * 128 + (b + 1) * chan_in, lane : lane + chan_mid] = tap

    wait_halo(1, pool.at[0], pool.at[slab2 - 1], poolh)
    for q, d in ((0, 0), (1, slab2 + 1)):

        def body(r, q=q, d=d):
            put_pooled(d, r, small, poolh[q, at(r, small), :].astype(F32))

        loop(rows2 // small, body)

    def col_sum(x):
        return x.reshape(x.shape[0] // 8, 8, x.shape[1]).sum(axis=0)

    gb2s[...] = jnp.zeros(gb2s.shape, F32)
    gb1s[...] = jnp.zeros(gb1s.shape, F32)
    for e in range(slab2):

        def body(r, e=e):
            pre = pre2[e, at(r, big), :] + b2s[0:1, :]
            if e == 0:
                pre = pre + dot(taps(p2, [0], r, big, (0, 1, 2)), k2[0:768, :])
            if e == slab2 - 1:
                pre = pre + dot(taps(p2, [slab2 + 1], r, big, (0, 1, 2)), k2[1536:2304, :])
            cots = jnp.concatenate([cotr[e, 0, at(r, big), :], cotr[e, 1, at(r, big), :]], axis=1)
            delta = cots * slope(pre)
            low = delta.astype(BF16)
            d2[e, at(r, big, wide), 0:256] = low
            d2[e, at(r, big, wide), 256:384] = from_right(delta[:, 0:128], wide).astype(BF16)
            d2[e, at(r, big, wide), 384:512] = from_left(delta[:, 128:256], wide).astype(BF16)
            rounded = low.astype(F32)
            gb2s[...] += col_sum(rounded)
            pre2[e, at(r, big), :] = rounded

        loop(rows2 // big, body)
        d2t[:, e * rows2 : (e + 1) * rows2] = pre2[e].T.astype(BF16)

    for e in range(slab2):

        def body(r, e=e):
            out = dot_t(taps(d2, [e], r, big, (2, 1, 0)), g2[...])
            for k in range(3):
                part = out[:, k * 128 : (k + 1) * 128]
                first = k == 2 or e == 0
                gp[e + k, at(r, big), :] = part if first else gp[e + k, at(r, big), :] + part

        loop(rows2 // big, body)

    gps[0] = gp[0].astype(BF16)
    gps[1] = gp[slab2 + 1].astype(BF16)
    send_halo(2, gps.at[0], gps.at[1], gpr)

    for k in range(3):
        for j in range(3):
            acc = None
            for e in range(slab2):
                one = dot(d2t[:, e * rows2 : (e + 1) * rows2], p2[e + k, j * wide : j * wide + rows2, :])
                acc = one if acc is None else acc + one
            t0, t1 = pltpu.roll(acc[0:128, 0:128], 64, 1), pltpu.roll(acc[0:128, 128:256], 64, 1)
            low = lanes(t0.shape) < 64
            f0 = jnp.where(low, t1, t0) + acc[128:256, 0:128]
            f1 = jnp.where(low, t0, t1) + acc[128:256, 128:256]
            base = (k * 3 + j) * 192
            s2x[base : base + 128, :] = f0.T.astype(BF16)
            s2x[base + 128 : base + 192, :] = f1.T[0:64, :].astype(BF16)
    bias = gb2s[...].sum(axis=0, keepdims=True)
    bias = bias[:, 0:128] + bias[:, 128:256]
    s2x[1728:1744, :] = jnp.broadcast_to(bias, (16, 128)).astype(BF16)
    if s2x.shape[0] > 1744:
        s2x[1744 : s2x.shape[0], :] = jnp.zeros((s2x.shape[0] - 1744, 128), BF16)

    sum2 = Sum(n, m, me, my, each2, s2x, s2got, s2part, s2gots, s2out, s2acc, (dsend2, drecv2, zsend2, zrecv2))
    sum1 = Sum(n, m, me, my, each1, s1x, s1got, s1part, s1gots, s1out, s1acc, (dsend1, drecv1, zsend1, zrecv1))
    sum2.step1()

    wait_halo(2, gps.at[0], gps.at[1], gpr)
    for e in range(slab2):

        def body(r, e=e):
            total = gp[e + 1, at(r, small // 2), :]
            if e == 0:
                total = total + gpr[0, at(r, small // 2), :].astype(F32)
            if e == slab2 - 1:
                total = total + gpr[1, at(r, small // 2), :].astype(F32)
            total = total * 0.125
            turned = pltpu.roll(total, 64, 1)
            low = lanes(total.shape) < 64
            both = jnp.concatenate([jnp.where(low, total, turned), jnp.where(low, turned, total)], axis=1)
            both = both.reshape(small // 2 // wide, 1, wide, 256)
            both = jnp.broadcast_to(both, (small // 2 // wide, 2, wide, 256)).reshape(small, 256)
            for d in (2 * e, 2 * e + 1):
                delta = both * slope(pre1[d, at(r, small), :])
                low_delta = delta.astype(BF16)
                d1[d, at(r, small, wide), 0:256] = low_delta
                edge = jnp.where(
                    lanes((small, 128)) < 64,
                    from_right(delta[:, 0:128], wide),
                    from_left(delta[:, 128:256], wide),
                )
                d1[d, at(r, small, wide), 256:384] = edge.astype(BF16)
                rounded = low_delta.astype(F32)
                gb1s[...] += col_sum(rounded)
                pre1[d, at(r, small), :] = rounded

        loop(rows // small, body)
    for d in range(slab):
        d1t[:, d * rows : (d + 1) * rows] = pre1[d].T.astype(BF16)
    sum2.step2()

    for k in range(3):
        for j in range(3):
            acc = None
            for d in range(slab):
                one = dot(d1t[:, d * rows : (d + 1) * rows], x2[d + k, j * wide : j * wide + rows, :])
                acc = one if acc is None else acc + one
            low = lanes((64, 128))
            total = acc[64:128, 0:128]
            total = total + jnp.where(
                low < 32, pltpu.roll(acc[0:64, 128:256], 32, 1), pltpu.roll(acc[0:64, 0:128], 32, 1)
            )
            total = total + pltpu.roll(acc[128:192, 0:128], 96, 1)
            total = total + jnp.where(
                low < 64, pltpu.roll(acc[192:256, 0:128], 64, 1), pltpu.roll(acc[192:256, 128:256], 64, 1)
            )
            t = k * 3 + j
            fold1[t % 5, (t // 5) * 64 : (t // 5) * 64 + 64, :] = total
        if k == 0:
            sum2.step3()
    fold1[4, 64:128, :] = jnp.zeros((64, 128), F32)
    for t in range(5):
        s1x[t * 96 : t * 96 + 96, :] = fold1[t].T[0:96, :].astype(BF16)
    bias = gb1s[...].sum(axis=0, keepdims=True)
    bias = bias[:, 0:128] + bias[:, 128:256]
    bias = bias + pltpu.roll(bias, 64, 1)
    s1x[480:496, :] = jnp.broadcast_to(bias, (16, 128)).astype(BF16)
    if s1x.shape[0] > 496:
        s1x[496 : s1x.shape[0], :] = jnp.zeros((s1x.shape[0] - 496, 128), BF16)
    sum1.step1()
    sum2.step4()

    for d in range(slab):

        def body(r, d=d):
            out = dot_t(taps(d1, [d], r, big, (2, 1, 0)), g1[...])
            for k in range(3):
                part = out[:, k * 128 : (k + 1) * 128]
                first = k == 2 or d == 0
                gx[d + k, at(r, big), :] = part if first else gx[d + k, at(r, big), :] + part

        loop(rows // big, body)
    gxs[0] = gx[0].astype(BF16)
    gxs[1] = gx[slab + 1].astype(BF16)
    send_halo(3, gxs.at[0], gxs.at[1], gxr)
    sum1.step2()
    sum2.step5()
    for t in range(9):
        gw2[t] = s2out[t * 192 : (t + 1) * 192, :].astype(F32) * scale_two
    gb2[...] = s2out[1728:1744, :].astype(F32)[0:1, :] * scale_two
    sum1.step3()
    wait_halo(3, gxs.at[0], gxs.at[1], gxr)
    for d in range(slab):
        total = gx[d + 1]
        if d == 0:
            total = total + gxr[0].astype(F32)
        if d == slab - 1:
            total = total + gxr[1].astype(F32)
        xr[...] = total
        for g in range(wide):
            gin[0, d, :, g * 128 : (g + 1) * 128] = xr[pl.ds(g, side, stride=wide), :].astype(BF16)
    sum1.step4()
    sum1.step5()
    for t in range(9):
        block = s1out[(t % 5) * 96 : (t % 5) * 96 + 96, :].astype(F32) * scale_one
        gw1[t] = block[:, (t // 5) * 64 : (t // 5) * 64 + 64]
    gb1[...] = s1out[480:496, :].astype(F32)[0:1, 0:64] * scale_one


def local(n, m, act_in, weight_one, bias_one, weight_two, bias_two, cotangent):
    samples, slab, side, merged = act_in.shape
    chan_in, chan_mid = weight_one.shape[3:]
    chan_out = weight_two.shape[4]
    slab2, half = cotangent.shape[1:3]
    assert samples == 1 and (chan_in, chan_mid, chan_out) == (32, 64, 128)
    scale_one = 16.0 / math.sqrt(samples * n * slab * m * side * side)
    scale_two = 1.0 / math.sqrt(samples * n * slab2 * m * half * half)
    wide = merged // 128
    rows, rows2 = side * wide, half * wide
    each = [-(-count // (n * m * 16)) * 16 for count in (496, 1744)]
    vmem = pltpu.VMEM

    def sums(size):
        return [
            vmem((n * m * size, 128), BF16),
            vmem((n, m * size, 128), BF16),
            vmem((m * size, 128), BF16),
            vmem((m, size, 128), BF16),
            vmem((n * m * size, 128), BF16),
            vmem((m * size, 128), F32),
        ]

    dma = pltpu.SemaphoreType.DMA
    spec = pl.BlockSpec(memory_space=pltpu.VMEM)
    outs = pl.pallas_call(
        functools.partial(kernel, n, m, scale_one, scale_two, each[0], each[1]),
        out_shape=[
            jax.ShapeDtypeStruct(act_in.shape, BF16),
            jax.ShapeDtypeStruct((9, 3 * chan_in, chan_mid), F32),
            jax.ShapeDtypeStruct((1, chan_mid), F32),
            jax.ShapeDtypeStruct((9, 3 * chan_mid, chan_out), F32),
            jax.ShapeDtypeStruct((1, chan_out), F32),
        ],
        in_specs=[spec] * 6,
        out_specs=[spec] * 5,
        scratch_shapes=[
            vmem((rows, 128), F32),
            vmem((slab + 2, rows + 2 * wide, 256), BF16),
            vmem((slab, rows, 256), F32),
            vmem((slab2, rows2, 128), BF16),
            vmem((slab2 + 2, rows2 + 2 * wide, 256), BF16),
            vmem((slab2, rows2, 256), F32),
            vmem((slab2, 2, rows2, 128), F32),
            vmem((slab2, rows2 + 2 * wide, 512), BF16),
            vmem((256, slab2 * rows2), BF16),
            vmem((slab2 + 2, rows2, 128), F32),
            vmem((slab, rows + 2 * wide, 384), BF16),
            vmem((256, slab * rows), BF16),
            vmem((slab + 2, rows, 128), F32),
            vmem((9 * 256, 256), BF16),
            vmem((9 * 256, 256), BF16),
            vmem((384, 3 * 384), BF16),
            vmem((384, 3 * 512), BF16),
            vmem((8, 256), F32),
            vmem((8, 256), F32),
            vmem((8, 256), F32),
            vmem((8, 256), F32),
            vmem((5, 128, 128), F32),
            vmem((2, side, merged), BF16),
            vmem((2, rows2, 128), BF16),
            vmem((2, rows2, 128), BF16),
            vmem((2, rows2, 128), BF16),
            vmem((2, rows, 128), BF16),
            vmem((2, rows, 128), BF16),
            *sums(each[1]),
            *sums(each[0]),
            dma((8,)),
            dma((8,)),
            dma((2 * n,)),
            dma((2 * n,)),
            dma((2 * m,)),
            dma((2 * m,)),
            dma((2 * n,)),
            dma((2 * n,)),
            dma((2 * m,)),
            dma((2 * m,)),
        ],
        compiler_params=pltpu.CompilerParams(
            collective_id=0, has_side_effects=True, vmem_limit_bytes=60 * 1024 * 1024
        ),
    )(
        act_in,
        weight_one.reshape(27, chan_in, chan_mid),
        bias_one.reshape(1, chan_mid),
        weight_two.reshape(27, chan_mid, chan_out),
        bias_two.reshape(1, chan_out),
        cotangent,
    )
    return (
        outs[0],
        outs[1].reshape(weight_one.shape),
        outs[2].reshape(bias_one.shape),
        outs[3].reshape(weight_two.shape),
        outs[4].reshape(bias_two.shape),
    )


def solution(mesh):
    placed = (P("dp", "space", None, None), P(), P(), P(), P(), P("dp", "space", None, None))
    return jax.shard_map(
        functools.partial(local, mesh.shape["dp"], mesh.shape["space"]),
        mesh=mesh,
        in_specs=placed,
        out_specs=(P("dp", "space", None, None), P(), P(), P(), P()),
        check_vma=False,
    )
```

```python
import functools
import math

import jax
import jax.numpy as jnp
from jax import lax
from jax.experimental import pallas as pl
from jax.experimental.pallas import tpu as pltpu
from jax.sharding import PartitionSpec as P

MESH = pl.DeviceIdType.MESH
F32 = jnp.float32
BF16 = jnp.bfloat16


def dot(a, b):
    return lax.dot_general(a, b, (((1,), (0,)), ((), ())), preferred_element_type=F32)


def dot_t(a, b):
    return lax.dot_general(a, b, (((1,), (1,)), ((), ())), preferred_element_type=F32)


def sigmoid(x):
    return 0.5 * jnp.tanh(0.5 * x) + 0.5


def slope(x):
    s = sigmoid(x)
    return s * (1.0 + x * (1.0 - s))


def lanes(shape):
    return lax.broadcasted_iota(jnp.int32, shape, 1)


def from_left(x, wide):
    g = lax.broadcasted_iota(jnp.int32, x.shape, 0) % wide
    return jnp.where(g == 0, 0.0, pltpu.roll(x, 1, 0))


def from_right(x, wide):
    g = lax.broadcasted_iota(jnp.int32, x.shape, 0) % wide
    return jnp.where(g == wide - 1, 0.0, pltpu.roll(x, x.shape[0] - 1, 0))


def edge_lanes(x, wide):
    return jnp.where(lanes(x.shape) < 64, from_right(x, wide), from_left(x, wide))


class Sum:
    def __init__(self, n, m, me, my, each, x, got, part, gots, out, acc, sems):
        self.n, self.m, self.me, self.my, self.each = n, m, me, my, each
        self.x, self.got, self.part, self.gots, self.out, self.acc = x, got, part, gots, out, acc
        self.send, self.recv, self.send_s, self.recv_s = sems

    def rows(self, count, start):
        return pl.ds(pl.multiple_of(start * self.each, 16), count * self.each)

    def to_dp(self, k, src, dst, base):
        return pltpu.make_async_remote_copy(
            src_ref=src,
            dst_ref=dst,
            send_sem=self.send.at[base + k],
            recv_sem=self.recv.at[base + k],
            device_id=(lax.rem(self.me + k, self.n), self.my),
            device_id_type=MESH,
        )

    def to_space(self, k, src, dst, base):
        return pltpu.make_async_remote_copy(
            src_ref=src,
            dst_ref=dst,
            send_sem=self.send_s.at[base + k],
            recv_sem=self.recv_s.at[base + k],
            device_id=(self.me, lax.rem(self.my + k, self.m)),
            device_id_type=MESH,
        )

    def step1(self):
        n, m = self.n, self.m
        self.c1 = []
        for k in range(1, n):
            src = self.x.at[self.rows(m, lax.rem(self.me + k, n) * m)]
            self.c1.append(self.to_dp(k, src, self.got.at[k], 0))
        for c in self.c1:
            c.start()

    def step2(self):
        n, m, each = self.n, self.m, self.each
        for c in self.c1:
            c.wait_recv()
        total = self.x[self.rows(m, self.me * m), :].astype(F32)
        for k in range(1, n):
            total = total + self.got[k].astype(F32)
        self.acc[...] = total
        self.part[...] = total.astype(BF16)
        self.c2 = []
        for k in range(1, m):
            src = self.part.at[self.rows(1, lax.rem(self.my + k, m))]
            self.c2.append(self.to_space(k, src, self.gots.at[k], 0))
        for c in self.c2:
            c.start()
        for c in self.c1:
            c.wait_send()

    def step3(self):
        m = self.m
        for c in self.c2:
            c.wait_recv()
        total = self.acc[self.rows(1, self.my), :]
        for k in range(1, m):
            total = total + self.gots[k].astype(F32)
        mine = self.rows(1, self.me * m + self.my)
        self.out[mine, :] = total.astype(BF16)
        self.c3 = [self.to_space(k, self.out.at[mine], self.out.at[mine], m) for k in range(1, m)]
        for c in self.c3:
            c.start()
        for c in self.c2:
            c.wait_send()

    def step4(self):
        n, m = self.n, self.m
        for c in self.c3:
            c.wait_recv()
        mine = self.rows(m, self.me * m)
        self.c4 = [self.to_dp(k, self.out.at[mine], self.out.at[mine], n) for k in range(1, n)]
        for c in self.c4:
            c.start()
        for c in self.c3:
            c.wait_send()

    def step5(self):
        for c in self.c4:
            c.wait_recv()
        for c in self.c4:
            c.wait_send()


class ShortSum(Sum):
    def step2(self):
        n, m = self.n, self.m
        for c in self.c1:
            c.wait_recv()
        total = self.x[self.rows(m, self.me * m), :].astype(F32)
        for k in range(1, n):
            total = total + self.got[k].astype(F32)
        low = total.astype(BF16)
        self.part[...] = low
        self.gots[self.my] = low
        self.c2 = [self.to_space(k, self.part, self.gots.at[self.my], 0) for k in range(1, m)]
        for c in self.c2:
            c.start()
        for c in self.c1:
            c.wait_send()

    def step3(self):
        n, m = self.n, self.m
        for c in self.c2:
            c.wait_recv()
        total = self.gots[0].astype(F32)
        for k in range(1, m):
            total = total + self.gots[k].astype(F32)
        mine = self.rows(m, self.me * m)
        self.out[mine, :] = total.astype(BF16)
        self.c4 = [self.to_dp(k, self.out.at[mine], self.out.at[mine], n) for k in range(1, n)]
        for c in self.c4:
            c.start()
        for c in self.c2:
            c.wait_send()


def kernel(
    n, m, scale_one, scale_two, each1, each2,
    act, w1, b1, w2, b2, cot,
    gin, gw1, gb1, gw2, gb2,
    xr, x2, pre1, pool, p2, pre2, cotr, d2, d2t, gp, d1, d1t, gx,
    k1, k2, g1, g2, b1s, b2s, gb1s, gb2s, fold1,
    acth, poolh, gps, gpr, gxs, gxr,
    s2x, s2got, s2part, s2gots, s2out, s2acc,
    s1x, s1got, s1part, s1gots, s1out, s1acc,
    hsend, hrecv, dsend2, drecv2, zsend2, zrecv2, dsend1, drecv1, zsend1, zrecv1,
):
    me = lax.axis_index("dp")
    my = lax.axis_index("space")
    slab, side, merged = act.shape[1:]
    wide = merged // 128
    slab2, half = cot.shape[1:3]
    rows, rows2 = side * wide, half * wide
    chan_in, chan_mid = w1.shape[1:]
    chan_out = w2.shape[2]
    big = min(512, rows2)
    small = 256

    barrier = pltpu.get_barrier_semaphore()
    for k in range(1, n):
        pl.semaphore_signal(barrier, inc=1, device_id=(lax.rem(me + k, n), my), device_id_type=MESH)
    for k in range(1, m):
        pl.semaphore_signal(barrier, inc=1, device_id=(me, lax.rem(my + k, m)), device_id_type=MESH)

    def loop(count, body):
        if count == 1:
            body(0)
        else:
            lax.fori_loop(0, count, lambda i, c: (body(i), c)[1], 0)

    def at(i, size, shift=0):
        return pl.ds(pl.multiple_of(i * size + shift, 16), size)

    def down(e, first, above):
        return pltpu.make_async_remote_copy(
            src_ref=first, dst_ref=above, send_sem=hsend.at[2 * e], recv_sem=hrecv.at[2 * e],
            device_id=(me, jnp.maximum(my - 1, 0)), device_id_type=MESH,
        )

    def up(e, last, below):
        return pltpu.make_async_remote_copy(
            src_ref=last, dst_ref=below, send_sem=hsend.at[2 * e + 1], recv_sem=hrecv.at[2 * e + 1],
            device_id=(me, jnp.minimum(my + 1, m - 1)), device_id_type=MESH,
        )

    def send_down(e, first, last, below, above):
        @pl.when(my > 0)
        def _():
            down(e, first, above).start()

    def send_up(e, first, last, below, above):
        @pl.when(my < m - 1)
        def _():
            up(e, last, below).start()

    def send_halo(e, *refs):
        send_down(e, *refs)
        send_up(e, *refs)

    def wait_halo(e, first, last, below, above):
        @pl.when(my > 0)
        def _():
            up(e, last, below).wait_recv()
            down(e, first, above).wait_send()

        @pl.when(my < m - 1)
        def _():
            down(e, first, above).wait_recv()
            up(e, last, below).wait_send()

        @pl.when(my == 0)
        def _():
            below[...] = jnp.zeros(below.shape, below.dtype)

        @pl.when(my == m - 1)
        def _():
            above[...] = jnp.zeros(above.shape, above.dtype)

    cuts = (0, side * 3 // 4, side)

    def act_halo(c):
        part = pl.ds(cuts[c], cuts[c + 1] - cuts[c])
        return act.at[0, 0, part], act.at[0, slab - 1, part], acth.at[0, part], acth.at[1, part]

    def half_halo(c, first, last, got):
        part = pl.ds(c * (rows2 // 2), rows2 // 2)
        return first.at[part], last.at[part], got.at[0, part], got.at[1, part]

    def pool_halo(c):
        return half_halo(c, pool.at[0], pool.at[slab2 - 1], poolh)

    def gp_halo(c):
        return half_halo(c, gps.at[0], gps.at[1], gpr)

    gx_halo = (gxs.at[0], gxs.at[1], gxr.at[0], gxr.at[1])

    k1[...] = jnp.zeros(k1.shape, BF16)
    for k in range(3):
        for j in range(3):
            for i in range(3):
                tap = w1[(k * 3 + j) * 3 + i]
                for b in range(4):
                    row = ((b + i - 1) * chan_in) % 256 + (k * 3 + j) * 256
                    k1[row : row + chan_in, b * chan_mid : (b + 1) * chan_mid] = tap

    for b in range(4):
        b1s[0:1, b * chan_mid : (b + 1) * chan_mid] = b1[...]
    for b in range(2):
        b2s[0:1, b * chan_out : (b + 1) * chan_out] = b2[...]

    pl.semaphore_wait(barrier, n + m - 2)
    for c in range(2):
        send_halo(c, *act_halo(c))

    def clear_edges(ref, planes, count):
        for d in range(planes):
            ref[d, 0:wide, :] = jnp.zeros((wide, ref.shape[2]), BF16)
            ref[d, count + wide : count + 2 * wide, :] = jnp.zeros((wide, ref.shape[2]), BF16)

    clear_edges(x2, slab + 2, rows)
    clear_edges(p2, slab2 + 2, rows2)
    clear_edges(d2, slab2, rows2)
    clear_edges(d1, slab, rows)

    def load_plane(src, d, start, stop):
        for g in range(wide):
            to = pl.ds(start * wide + g, stop - start, stride=wide)
            xr[to, :] = src[start:stop, g * 128 : (g + 1) * 128].astype(F32)
        skip = start * wide

        def body(r):
            main = xr[at(r, small, skip), :]
            x2[d, at(r, small, skip + wide), 0:128] = main.astype(BF16)
            x2[d, at(r, small, skip + wide), 128:256] = edge_lanes(main, wide).astype(BF16)

        loop((stop - start) * wide // small, body)

    for d in range(slab):
        load_plane(act.at[0, d], d + 1, 0, side)

    def taps(ref, planes, r, size, shifts):
        return jnp.concatenate([ref[p, at(r, size, s * wide), :] for p in planes for s in shifts], axis=1)

    for d in range(slab):
        ks = [k for k in range(3) if 0 <= d + k - 1 < slab]

        def body(r, d=d, ks=ks):
            left = taps(x2, [d + k for k in ks], r, big, (0, 1, 2))
            pre1[d, at(r, big), :] = dot(left, k1[ks[0] * 768 : (ks[-1] + 1) * 768, :])

        loop(rows // big, body)

    k2[...] = jnp.zeros(k2.shape, BF16)
    for k in range(3):
        for j in range(3):
            for i in range(3):
                tap = w2[(k * 3 + j) * 3 + i]
                for b in range(2):
                    row = ((b + i - 1) * chan_mid) % 256 + (k * 3 + j) * 256
                    k2[row : row + chan_mid, b * chan_out : (b + 1) * chan_out] = tap
    for d in range(slab2):
        for g in range(wide):
            for t in range(2):
                cotr[d, t, pl.ds(g, half, stride=wide), :] = cot[0, d, :, g * 256 + t * 128 : g * 256 + t * 128 + 128].astype(F32)

    def put_pooled(d, r, size, main):
        p2[d, at(r, size, wide), 0:128] = main.astype(BF16)
        p2[d, at(r, size, wide), 128:256] = edge_lanes(main, wide).astype(BF16)

    for part in range(2):
        wait_halo(part, *act_halo(part))
        load_plane(acth.at[0], 0, cuts[part], cuts[part + 1])
        load_plane(acth.at[1], slab + 1, cuts[part], cuts[part + 1])
        for e in range(slab2):

            def body(r, e=e, part=part):
                r = r + part * (rows // 2 // big)
                total = None
                for d in (2 * e, 2 * e + 1):
                    pre = pre1[d, at(r, big), :] + b1s[0:1, :]
                    if d == 0:
                        pre = pre + dot(taps(x2, [0], r, big, (0, 1, 2)), k1[0:768, :])
                    if d == slab - 1:
                        pre = pre + dot(taps(x2, [slab + 1], r, big, (0, 1, 2)), k1[1536:2304, :])
                    pre1[d, at(r, big), :] = pre
                    one = pre * sigmoid(pre)
                    total = one if total is None else total + one
                pairs = total.reshape(big // (2 * wide), 2, wide, 256)
                quad = (pairs[:, 0] + pairs[:, 1]).reshape(big // 2, 256)
                a, b = quad[:, 0:128], quad[:, 128:256]
                a = a + pltpu.roll(a, 64, 1)
                b = b + pltpu.roll(b, 64, 1)
                mean = (jnp.where(lanes(a.shape) < 64, a, b) * 0.125).astype(BF16)
                pool[e, at(r, big // 2), :] = mean
                put_pooled(e + 1, r, big // 2, mean.astype(F32))

            loop(rows // 2 // big, body)
        send_halo(2 + part, *pool_halo(part))

    for e in range(slab2):
        ks = [k for k in range(3) if 0 <= e + k - 1 < slab2]

        def body(r, e=e, ks=ks):
            left = taps(p2, [e + k for k in ks], r, big, (0, 1, 2))
            pre2[e, at(r, big), :] = dot(left, k2[ks[0] * 768 : (ks[-1] + 1) * 768, :])

        loop(rows2 // big, body)

    g2[...] = jnp.zeros(g2.shape, BF16)
    g1[...] = jnp.zeros(g1.shape, BF16)
    for k in range(3):
        for j in range(3):
            for i in range(3):
                tap = w2[(k * 3 + j) * 3 + i]
                for b in range(2):
                    lane = j * 512 + ((b - i + 1) * chan_out) % 512
                    g2[k * 128 + b * chan_mid : k * 128 + (b + 1) * chan_mid, lane : lane + chan_out] = tap
                tap = w1[(k * 3 + j) * 3 + i]
                for b in range(4):
                    lane = j * 384 + ((b - i + 1) * chan_mid) % 384
                    g1[k * 128 + b * chan_in : k * 128 + (b + 1) * chan_in, lane : lane + chan_mid] = tap

    for c in range(2):
        wait_halo(2 + c, *pool_halo(c))
    for q, d in ((0, 0), (1, slab2 + 1)):

        def body(r, q=q, d=d):
            put_pooled(d, r, small, poolh[q, at(r, small), :].astype(F32))

        loop(rows2 // small, body)

    def col_sum(x):
        return x.reshape(x.shape[0] // 8, 8, x.shape[1]).sum(axis=0)

    gb2s[...] = jnp.zeros(gb2s.shape, F32)
    gb1s[...] = jnp.zeros(gb1s.shape, F32)
    for e in range(slab2):

        def body(r, e=e):
            pre = pre2[e, at(r, big), :] + b2s[0:1, :]
            if e == 0:
                pre = pre + dot(taps(p2, [0], r, big, (0, 1, 2)), k2[0:768, :])
            if e == slab2 - 1:
                pre = pre + dot(taps(p2, [slab2 + 1], r, big, (0, 1, 2)), k2[1536:2304, :])
            cots = jnp.concatenate([cotr[e, 0, at(r, big), :], cotr[e, 1, at(r, big), :]], axis=1)
            delta = cots * slope(pre)
            low = delta.astype(BF16)
            d2[e, at(r, big, wide), 0:256] = low
            d2[e, at(r, big, wide), 256:384] = from_right(delta[:, 0:128], wide).astype(BF16)
            d2[e, at(r, big, wide), 384:512] = from_left(delta[:, 128:256], wide).astype(BF16)
            rounded = low.astype(F32)
            gb2s[...] += col_sum(rounded)
            pre2[e, at(r, big), :] = rounded

        loop(rows2 // big, body)
        d2t[:, e * rows2 : (e + 1) * rows2] = pre2[e].T.astype(BF16)

    for e in range(slab2):

        def body(r, e=e):
            out = dot_t(taps(d2, [e], r, big, (2, 1, 0)), g2[...])
            for k in range(3):
                part = out[:, k * 128 : (k + 1) * 128]
                first = k == 2 or e == 0
                gp[e + k, at(r, big), :] = part if first else gp[e + k, at(r, big), :] + part

        loop(rows2 // big, body)

    gps[0] = gp[0].astype(BF16)
    gps[1] = gp[slab2 + 1].astype(BF16)
    for c in range(2):
        send_halo(4 + c, *gp_halo(c))

    for k in range(3):
        for j in range(3):
            acc = None
            for e in range(slab2):
                one = dot(d2t[:, e * rows2 : (e + 1) * rows2], p2[e + k, j * wide : j * wide + rows2, :])
                acc = one if acc is None else acc + one
            t0, t1 = pltpu.roll(acc[0:128, 0:128], 64, 1), pltpu.roll(acc[0:128, 128:256], 64, 1)
            low = lanes(t0.shape) < 64
            f0 = jnp.where(low, t1, t0) + acc[128:256, 0:128]
            f1 = jnp.where(low, t0, t1) + acc[128:256, 128:256]
            base = (k * 3 + j) * 192
            s2x[base : base + 128, :] = f0.T.astype(BF16)
            s2x[base + 128 : base + 192, :] = f1.T[0:64, :].astype(BF16)
    bias = gb2s[...].sum(axis=0, keepdims=True)
    bias = bias[:, 0:128] + bias[:, 128:256]
    s2x[1728:1744, :] = jnp.broadcast_to(bias, (16, 128)).astype(BF16)
    if s2x.shape[0] > 1744:
        s2x[1744 : s2x.shape[0], :] = jnp.zeros((s2x.shape[0] - 1744, 128), BF16)

    sum2 = Sum(n, m, me, my, each2, s2x, s2got, s2part, s2gots, s2out, s2acc, (dsend2, drecv2, zsend2, zrecv2))
    sum1 = ShortSum(n, m, me, my, each1, s1x, s1got, s1part, s1gots, s1out, s1acc, (dsend1, drecv1, zsend1, zrecv1))
    sum2.step1()

    for c in range(2):
        wait_halo(4 + c, *gp_halo(c))
        for e in range(slab2):

            def body(r, e=e, c=c):
                r = r + c * (rows // 2 // small)
                total = gp[e + 1, at(r, small // 2), :]
                if e == 0:
                    total = total + gpr[0, at(r, small // 2), :].astype(F32)
                if e == slab2 - 1:
                    total = total + gpr[1, at(r, small // 2), :].astype(F32)
                total = total * 0.125
                turned = pltpu.roll(total, 64, 1)
                low = lanes(total.shape) < 64
                both = jnp.concatenate([jnp.where(low, total, turned), jnp.where(low, turned, total)], axis=1)
                both = both.reshape(small // 2 // wide, 1, wide, 256)
                both = jnp.broadcast_to(both, (small // 2 // wide, 2, wide, 256)).reshape(small, 256)
                for d in (2 * e, 2 * e + 1):
                    delta = both * slope(pre1[d, at(r, small), :])
                    low_delta = delta.astype(BF16)
                    d1[d, at(r, small, wide), 0:256] = low_delta
                    edge = jnp.where(
                        lanes((small, 128)) < 64,
                        from_right(delta[:, 0:128], wide),
                        from_left(delta[:, 128:256], wide),
                    )
                    d1[d, at(r, small, wide), 256:384] = edge.astype(BF16)
                    rounded = low_delta.astype(F32)
                    gb1s[...] += col_sum(rounded)
                    pre1[d, at(r, small), :] = rounded

            loop(rows // 2 // small, body)
    for d in range(slab):
        d1t[:, d * rows : (d + 1) * rows] = pre1[d].T.astype(BF16)

    for d in range(slab):

        def body(r, d=d):
            out = dot_t(taps(d1, [d], r, big, (2, 1, 0)), g1[...])
            for k in range(3):
                part = out[:, k * 128 : (k + 1) * 128]
                first = k == 2 or d == 0
                gx[d + k, at(r, big), :] = part if first else gx[d + k, at(r, big), :] + part

        loop(rows // big, body)
        if d == 0:
            gxs[0] = gx[0].astype(BF16)
    gxs[1] = gx[slab + 1].astype(BF16)
    sum2.step2()

    for k in range(3):
        for j in range(3):
            acc = None
            for d in range(slab):
                one = dot(d1t[:, d * rows : (d + 1) * rows], x2[d + k, j * wide : j * wide + rows, :])
                acc = one if acc is None else acc + one
            low = lanes((64, 128))
            total = acc[64:128, 0:128]
            total = total + jnp.where(
                low < 32, pltpu.roll(acc[0:64, 128:256], 32, 1), pltpu.roll(acc[0:64, 0:128], 32, 1)
            )
            total = total + pltpu.roll(acc[128:192, 0:128], 96, 1)
            total = total + jnp.where(
                low < 64, pltpu.roll(acc[192:256, 0:128], 64, 1), pltpu.roll(acc[192:256, 128:256], 64, 1)
            )
            t = k * 3 + j
            fold1[t % 5, (t // 5) * 64 : (t // 5) * 64 + 64, :] = total
    fold1[4, 64:128, :] = jnp.zeros((64, 128), F32)
    for t in range(5):
        s1x[t * 96 : t * 96 + 96, :] = fold1[t].T[0:96, :].astype(BF16)
    bias = gb1s[...].sum(axis=0, keepdims=True)
    bias = bias[:, 0:128] + bias[:, 128:256]
    bias = bias + pltpu.roll(bias, 64, 1)
    s1x[480:496, :] = jnp.broadcast_to(bias, (16, 128)).astype(BF16)
    if s1x.shape[0] > 496:
        s1x[496 : s1x.shape[0], :] = jnp.zeros((s1x.shape[0] - 496, 128), BF16)
    sum1.step1()
    sum2.step3()
    send_halo(6, *gx_halo)
    sum2.step4()
    sum1.step2()
    sum1.step3()
    wait_halo(6, *gx_halo)
    for d in range(slab):
        total = gx[d + 1]
        if d == 0:
            total = total + gxr[0].astype(F32)
        if d == slab - 1:
            total = total + gxr[1].astype(F32)
        xr[...] = total
        for g in range(wide):
            gin[0, d, :, g * 128 : (g + 1) * 128] = xr[pl.ds(g, side, stride=wide), :].astype(BF16)
    sum2.step5()
    for t in range(9):
        gw2[t] = s2out[t * 192 : (t + 1) * 192, :].astype(F32) * scale_two
    gb2[...] = s2out[1728:1744, :].astype(F32)[0:1, :] * scale_two
    sum1.step5()
    for t in range(9):
        block = s1out[(t % 5) * 96 : (t % 5) * 96 + 96, :].astype(F32) * scale_one
        gw1[t] = block[:, (t // 5) * 64 : (t // 5) * 64 + 64]
    gb1[...] = s1out[480:496, :].astype(F32)[0:1, 0:64] * scale_one


def local(n, m, act_in, weight_one, bias_one, weight_two, bias_two, cotangent):
    samples, slab, side, merged = act_in.shape
    chan_in, chan_mid = weight_one.shape[3:]
    chan_out = weight_two.shape[4]
    slab2, half = cotangent.shape[1:3]
    assert samples == 1 and (chan_in, chan_mid, chan_out) == (32, 64, 128)
    scale_one = 16.0 / math.sqrt(samples * n * slab * m * side * side)
    scale_two = 1.0 / math.sqrt(samples * n * slab2 * m * half * half)
    wide = merged // 128
    rows, rows2 = side * wide, half * wide
    each = [-(-count // (n * m * 16)) * 16 for count in (496, 1744)]
    vmem = pltpu.VMEM

    def sums(size, slots):
        return [
            vmem((n * m * size, 128), BF16),
            vmem((n, m * size, 128), BF16),
            vmem((m * size, 128), BF16),
            vmem((m, slots * size, 128), BF16),
            vmem((n * m * size, 128), BF16),
            vmem((m * size, 128), F32),
        ]

    dma = pltpu.SemaphoreType.DMA
    spec = pl.BlockSpec(memory_space=pltpu.VMEM)
    outs = pl.pallas_call(
        functools.partial(kernel, n, m, scale_one, scale_two, each[0], each[1]),
        out_shape=[
            jax.ShapeDtypeStruct(act_in.shape, BF16),
            jax.ShapeDtypeStruct((9, 3 * chan_in, chan_mid), F32),
            jax.ShapeDtypeStruct((1, chan_mid), F32),
            jax.ShapeDtypeStruct((9, 3 * chan_mid, chan_out), F32),
            jax.ShapeDtypeStruct((1, chan_out), F32),
        ],
        in_specs=[spec] * 6,
        out_specs=[spec] * 5,
        scratch_shapes=[
            vmem((rows, 128), F32),
            vmem((slab + 2, rows + 2 * wide, 256), BF16),
            vmem((slab, rows, 256), F32),
            vmem((slab2, rows2, 128), BF16),
            vmem((slab2 + 2, rows2 + 2 * wide, 256), BF16),
            vmem((slab2, rows2, 256), F32),
            vmem((slab2, 2, rows2, 128), F32),
            vmem((slab2, rows2 + 2 * wide, 512), BF16),
            vmem((256, slab2 * rows2), BF16),
            vmem((slab2 + 2, rows2, 128), F32),
            vmem((slab, rows + 2 * wide, 384), BF16),
            vmem((256, slab * rows), BF16),
            vmem((slab + 2, rows, 128), F32),
            vmem((9 * 256, 256), BF16),
            vmem((9 * 256, 256), BF16),
            vmem((384, 3 * 384), BF16),
            vmem((384, 3 * 512), BF16),
            vmem((8, 256), F32),
            vmem((8, 256), F32),
            vmem((8, 256), F32),
            vmem((8, 256), F32),
            vmem((5, 128, 128), F32),
            vmem((2, side, merged), BF16),
            vmem((2, rows2, 128), BF16),
            vmem((2, rows2, 128), BF16),
            vmem((2, rows2, 128), BF16),
            vmem((2, rows, 128), BF16),
            vmem((2, rows, 128), BF16),
            *sums(each[1], 1),
            *sums(each[0], m),
            dma((14,)),
            dma((14,)),
            dma((2 * n,)),
            dma((2 * n,)),
            dma((2 * m,)),
            dma((2 * m,)),
            dma((2 * n,)),
            dma((2 * n,)),
            dma((2 * m,)),
            dma((2 * m,)),
        ],
        compiler_params=pltpu.CompilerParams(
            collective_id=0, has_side_effects=True, vmem_limit_bytes=60 * 1024 * 1024
        ),
    )(
        act_in,
        weight_one.reshape(27, chan_in, chan_mid),
        bias_one.reshape(1, chan_mid),
        weight_two.reshape(27, chan_mid, chan_out),
        bias_two.reshape(1, chan_out),
        cotangent,
    )
    return (
        outs[0],
        outs[1].reshape(weight_one.shape),
        outs[2].reshape(bias_one.shape),
        outs[3].reshape(weight_two.shape),
        outs[4].reshape(bias_two.shape),
    )


def solution(mesh):
    placed = (P("dp", "space", None, None), P(), P(), P(), P(), P("dp", "space", None, None))
    return jax.shard_map(
        functools.partial(local, mesh.shape["dp"], mesh.shape["space"]),
        mesh=mesh,
        in_specs=placed,
        out_specs=(P("dp", "space", None, None), P(), P(), P(), P()),
        check_vma=False,
    )
```

```python
import functools
import math

import jax
import jax.numpy as jnp
from jax import lax
from jax.experimental import pallas as pl
from jax.experimental.pallas import tpu as pltpu
from jax.sharding import PartitionSpec as P

MESH = pl.DeviceIdType.MESH
F32 = jnp.float32
BF16 = jnp.bfloat16


def dot(a, b):
    return lax.dot_general(a, b, (((1,), (0,)), ((), ())), preferred_element_type=F32)


def dot_t(a, b):
    return lax.dot_general(a, b, (((1,), (1,)), ((), ())), preferred_element_type=F32)


def sigmoid(x):
    return 0.5 * jnp.tanh(0.5 * x) + 0.5


def slope(x):
    s = sigmoid(x)
    return s * (1.0 + x * (1.0 - s))


def lanes(shape):
    return lax.broadcasted_iota(jnp.int32, shape, 1)


def from_left(x, wide):
    g = lax.broadcasted_iota(jnp.int32, x.shape, 0) % wide
    return jnp.where(g == 0, 0.0, pltpu.roll(x, 1, 0))


def from_right(x, wide):
    g = lax.broadcasted_iota(jnp.int32, x.shape, 0) % wide
    return jnp.where(g == wide - 1, 0.0, pltpu.roll(x, x.shape[0] - 1, 0))


def edge_lanes(x, wide):
    return jnp.where(lanes(x.shape) < 64, from_right(x, wide), from_left(x, wide))


class Sum:
    def __init__(self, n, m, me, my, each, x, got, part, gots, out, acc, sems):
        self.n, self.m, self.me, self.my, self.each = n, m, me, my, each
        self.x, self.got, self.part, self.gots, self.out, self.acc = x, got, part, gots, out, acc
        self.send, self.recv, self.send_s, self.recv_s = sems

    def rows(self, count, start):
        return pl.ds(pl.multiple_of(start * self.each, 16), count * self.each)

    def to_dp(self, k, src, dst, base):
        return pltpu.make_async_remote_copy(
            src_ref=src,
            dst_ref=dst,
            send_sem=self.send.at[base + k],
            recv_sem=self.recv.at[base + k],
            device_id=(lax.rem(self.me + k, self.n), self.my),
            device_id_type=MESH,
        )

    def to_space(self, k, src, dst, base):
        return pltpu.make_async_remote_copy(
            src_ref=src,
            dst_ref=dst,
            send_sem=self.send_s.at[base + k],
            recv_sem=self.recv_s.at[base + k],
            device_id=(self.me, lax.rem(self.my + k, self.m)),
            device_id_type=MESH,
        )

    def step1(self):
        n, m = self.n, self.m
        self.c1 = []
        for k in range(1, n):
            src = self.x.at[self.rows(m, lax.rem(self.me + k, n) * m)]
            self.c1.append(self.to_dp(k, src, self.got.at[k], 0))
        for c in self.c1:
            c.start()

    def step2(self):
        n, m, each = self.n, self.m, self.each
        for c in self.c1:
            c.wait_recv()
        total = self.x[self.rows(m, self.me * m), :].astype(F32)
        for k in range(1, n):
            total = total + self.got[k].astype(F32)
        self.acc[...] = total
        self.part[...] = total.astype(BF16)
        self.c2 = []
        for k in range(1, m):
            src = self.part.at[self.rows(1, lax.rem(self.my + k, m))]
            self.c2.append(self.to_space(k, src, self.gots.at[k], 0))
        for c in self.c2:
            c.start()
        for c in self.c1:
            c.wait_send()

    def step3(self):
        m = self.m
        for c in self.c2:
            c.wait_recv()
        total = self.acc[self.rows(1, self.my), :]
        for k in range(1, m):
            total = total + self.gots[k].astype(F32)
        mine = self.rows(1, self.me * m + self.my)
        self.out[mine, :] = total.astype(BF16)
        self.c3 = [self.to_space(k, self.out.at[mine], self.out.at[mine], m) for k in range(1, m)]
        for c in self.c3:
            c.start()
        for c in self.c2:
            c.wait_send()

    def step4(self):
        n, m = self.n, self.m
        for c in self.c3:
            c.wait_recv()
        mine = self.rows(m, self.me * m)
        self.c4 = [self.to_dp(k, self.out.at[mine], self.out.at[mine], n) for k in range(1, n)]
        for c in self.c4:
            c.start()
        for c in self.c3:
            c.wait_send()

    def step5(self):
        for c in self.c4:
            c.wait_recv()
        for c in self.c4:
            c.wait_send()


class ShortSum(Sum):
    def step2(self):
        n, m = self.n, self.m
        for c in self.c1:
            c.wait_recv()
        total = self.x[self.rows(m, self.me * m), :].astype(F32)
        for k in range(1, n):
            total = total + self.got[k].astype(F32)
        low = total.astype(BF16)
        self.part[...] = low
        self.gots[self.my] = low
        self.c2 = [self.to_space(k, self.part, self.gots.at[self.my], 0) for k in range(1, m)]
        for c in self.c2:
            c.start()
        for c in self.c1:
            c.wait_send()

    def step3(self):
        n, m = self.n, self.m
        for c in self.c2:
            c.wait_recv()
        total = self.gots[0].astype(F32)
        for k in range(1, m):
            total = total + self.gots[k].astype(F32)
        mine = self.rows(m, self.me * m)
        self.out[mine, :] = total.astype(BF16)
        self.c4 = [self.to_dp(k, self.out.at[mine], self.out.at[mine], n) for k in range(1, n)]
        for c in self.c4:
            c.start()
        for c in self.c2:
            c.wait_send()


def kernel(
    n, m, each1, each2,
    act, w1, b1, w2, b2, cot,
    gin, s1out, s2out,
    xr, x2, pre1, pool, p2, pre2, cotr, d2, d2t, gp, d1, d1t, gx,
    k1, k2, g1, g2, b1s, b2s, gb1s, gb2s, fold1,
    acth, poolh, gps, gpr, gxs, gxr,
    s2x, s2got, s2part, s2gots, s2acc,
    s1x, s1got, s1part, s1gots, s1acc,
    hsend, hrecv, dsend2, drecv2, zsend2, zrecv2, dsend1, drecv1, zsend1, zrecv1,
):
    me = lax.axis_index("dp")
    my = lax.axis_index("space")
    slab, side, merged = act.shape[1:]
    wide = merged // 128
    slab2, half = cot.shape[1:3]
    rows, rows2 = side * wide, half * wide
    chan_in, chan_mid = w1.shape[1:]
    chan_out = w2.shape[2]
    big = min(512, rows2)
    small = 256

    barrier = pltpu.get_barrier_semaphore()
    for k in range(1, n):
        pl.semaphore_signal(barrier, inc=1, device_id=(lax.rem(me + k, n), my), device_id_type=MESH)
    for k in range(1, m):
        pl.semaphore_signal(barrier, inc=1, device_id=(me, lax.rem(my + k, m)), device_id_type=MESH)

    def loop(count, body):
        if count == 1:
            body(0)
        else:
            lax.fori_loop(0, count, lambda i, c: (body(i), c)[1], 0)

    def at(i, size, shift=0):
        return pl.ds(pl.multiple_of(i * size + shift, 16), size)

    def down(e, first, above):
        return pltpu.make_async_remote_copy(
            src_ref=first, dst_ref=above, send_sem=hsend.at[2 * e], recv_sem=hrecv.at[2 * e],
            device_id=(me, jnp.maximum(my - 1, 0)), device_id_type=MESH,
        )

    def up(e, last, below):
        return pltpu.make_async_remote_copy(
            src_ref=last, dst_ref=below, send_sem=hsend.at[2 * e + 1], recv_sem=hrecv.at[2 * e + 1],
            device_id=(me, jnp.minimum(my + 1, m - 1)), device_id_type=MESH,
        )

    def send_down(e, first, last, below, above):
        @pl.when(my > 0)
        def _():
            down(e, first, above).start()

    def send_up(e, first, last, below, above):
        @pl.when(my < m - 1)
        def _():
            up(e, last, below).start()

    def send_halo(e, *refs):
        send_down(e, *refs)
        send_up(e, *refs)

    def wait_halo(e, first, last, below, above):
        @pl.when(my > 0)
        def _():
            up(e, last, below).wait_recv()
            down(e, first, above).wait_send()

        @pl.when(my < m - 1)
        def _():
            down(e, first, above).wait_recv()
            up(e, last, below).wait_send()

        @pl.when(my == 0)
        def _():
            below[...] = jnp.zeros(below.shape, below.dtype)

        @pl.when(my == m - 1)
        def _():
            above[...] = jnp.zeros(above.shape, above.dtype)

    cuts = (0, side * 3 // 4, side)

    def act_halo(c):
        part = pl.ds(cuts[c], cuts[c + 1] - cuts[c])
        return act.at[0, 0, part], act.at[0, slab - 1, part], acth.at[0, part], acth.at[1, part]

    def half_halo(c, first, last, got):
        part = pl.ds(c * (rows2 // 2), rows2 // 2)
        return first.at[part], last.at[part], got.at[0, part], got.at[1, part]

    def pool_halo(c):
        return half_halo(c, pool.at[0], pool.at[slab2 - 1], poolh)

    def gp_halo(c):
        return half_halo(c, gps.at[0], gps.at[1], gpr)

    gx_halo = (gxs.at[0], gxs.at[1], gxr.at[0], gxr.at[1])

    k1[...] = jnp.zeros(k1.shape, BF16)
    for k in range(3):
        for j in range(3):
            for i in range(3):
                tap = w1[(k * 3 + j) * 3 + i]
                for b in range(4):
                    row = ((b + i - 1) * chan_in) % 256 + (k * 3 + j) * 256
                    k1[row : row + chan_in, b * chan_mid : (b + 1) * chan_mid] = tap

    for b in range(4):
        b1s[0:1, b * chan_mid : (b + 1) * chan_mid] = b1[...]
    for b in range(2):
        b2s[0:1, b * chan_out : (b + 1) * chan_out] = b2[...]

    pl.semaphore_wait(barrier, n + m - 2)
    for c in range(2):
        send_halo(c, *act_halo(c))

    def clear_edges(ref, planes, count):
        for d in range(planes):
            ref[d, 0:wide, :] = jnp.zeros((wide, ref.shape[2]), BF16)
            ref[d, count + wide : count + 2 * wide, :] = jnp.zeros((wide, ref.shape[2]), BF16)

    clear_edges(x2, slab + 2, rows)
    clear_edges(p2, slab2 + 2, rows2)
    clear_edges(d2, slab2, rows2)
    clear_edges(d1, slab, rows)

    def load_plane(src, d, start, stop):
        for g in range(wide):
            to = pl.ds(start * wide + g, stop - start, stride=wide)
            xr[to, :] = src[start:stop, g * 128 : (g + 1) * 128].astype(F32)
        skip = start * wide

        def body(r):
            main = xr[at(r, small, skip), :]
            x2[d, at(r, small, skip + wide), 0:128] = main.astype(BF16)
            x2[d, at(r, small, skip + wide), 128:256] = edge_lanes(main, wide).astype(BF16)

        loop((stop - start) * wide // small, body)

    for d in range(slab):
        load_plane(act.at[0, d], d + 1, 0, side)

    def taps(ref, planes, r, size, shifts):
        return jnp.concatenate([ref[p, at(r, size, s * wide), :] for p in planes for s in shifts], axis=1)

    for d in range(slab):
        ks = [k for k in range(3) if 0 <= d + k - 1 < slab]

        def body(r, d=d, ks=ks):
            left = taps(x2, [d + k for k in ks], r, big, (0, 1, 2))
            pre1[d, at(r, big), :] = dot(left, k1[ks[0] * 768 : (ks[-1] + 1) * 768, :])

        loop(rows // big, body)

    k2[...] = jnp.zeros(k2.shape, BF16)
    for k in range(3):
        for j in range(3):
            for i in range(3):
                tap = w2[(k * 3 + j) * 3 + i]
                for b in range(2):
                    row = ((b + i - 1) * chan_mid) % 256 + (k * 3 + j) * 256
                    k2[row : row + chan_mid, b * chan_out : (b + 1) * chan_out] = tap
    for d in range(slab2):
        for g in range(wide):
            for t in range(2):
                cotr[d, t, pl.ds(g, half, stride=wide), :] = cot[0, d, :, g * 256 + t * 128 : g * 256 + t * 128 + 128].astype(F32)

    def put_pooled(d, r, size, main):
        p2[d, at(r, size, wide), 0:128] = main.astype(BF16)
        p2[d, at(r, size, wide), 128:256] = edge_lanes(main, wide).astype(BF16)

    for part in range(2):
        wait_halo(part, *act_halo(part))
        load_plane(acth.at[0], 0, cuts[part], cuts[part + 1])
        load_plane(acth.at[1], slab + 1, cuts[part], cuts[part + 1])
        for e in range(slab2):

            def body(r, e=e, part=part):
                r = r + part * (rows // 2 // big)
                total = None
                for d in (2 * e, 2 * e + 1):
                    pre = pre1[d, at(r, big), :] + b1s[0:1, :]
                    if d == 0:
                        pre = pre + dot(taps(x2, [0], r, big, (0, 1, 2)), k1[0:768, :])
                    if d == slab - 1:
                        pre = pre + dot(taps(x2, [slab + 1], r, big, (0, 1, 2)), k1[1536:2304, :])
                    pre1[d, at(r, big), :] = pre
                    one = pre * sigmoid(pre)
                    total = one if total is None else total + one
                pairs = total.reshape(big // (2 * wide), 2, wide, 256)
                quad = (pairs[:, 0] + pairs[:, 1]).reshape(big // 2, 256)
                a, b = quad[:, 0:128], quad[:, 128:256]
                a = a + pltpu.roll(a, 64, 1)
                b = b + pltpu.roll(b, 64, 1)
                mean = (jnp.where(lanes(a.shape) < 64, a, b) * 0.125).astype(BF16)
                pool[e, at(r, big // 2), :] = mean
                put_pooled(e + 1, r, big // 2, mean.astype(F32))

            loop(rows // 2 // big, body)
        send_halo(2 + part, *pool_halo(part))

    for e in range(slab2):
        ks = [k for k in range(3) if 0 <= e + k - 1 < slab2]

        def body(r, e=e, ks=ks):
            left = taps(p2, [e + k for k in ks], r, big, (0, 1, 2))
            pre2[e, at(r, big), :] = dot(left, k2[ks[0] * 768 : (ks[-1] + 1) * 768, :])

        loop(rows2 // big, body)

    g2[...] = jnp.zeros(g2.shape, BF16)
    g1[...] = jnp.zeros(g1.shape, BF16)
    for k in range(3):
        for j in range(3):
            for i in range(3):
                tap = w2[(k * 3 + j) * 3 + i]
                for b in range(2):
                    lane = j * 512 + ((b - i + 1) * chan_out) % 512
                    g2[k * 128 + b * chan_mid : k * 128 + (b + 1) * chan_mid, lane : lane + chan_out] = tap
                tap = w1[(k * 3 + j) * 3 + i]
                for b in range(4):
                    lane = j * 384 + ((b - i + 1) * chan_mid) % 384
                    g1[k * 128 + b * chan_in : k * 128 + (b + 1) * chan_in, lane : lane + chan_mid] = tap

    for c in range(2):
        wait_halo(2 + c, *pool_halo(c))
    for q, d in ((0, 0), (1, slab2 + 1)):

        def body(r, q=q, d=d):
            put_pooled(d, r, small, poolh[q, at(r, small), :].astype(F32))

        loop(rows2 // small, body)

    def col_sum(x):
        return x.reshape(x.shape[0] // 8, 8, x.shape[1]).sum(axis=0)

    gb2s[...] = jnp.zeros(gb2s.shape, F32)
    gb1s[...] = jnp.zeros(gb1s.shape, F32)
    for e in range(slab2):

        def body(r, e=e):
            pre = pre2[e, at(r, big), :] + b2s[0:1, :]
            if e == 0:
                pre = pre + dot(taps(p2, [0], r, big, (0, 1, 2)), k2[0:768, :])
            if e == slab2 - 1:
                pre = pre + dot(taps(p2, [slab2 + 1], r, big, (0, 1, 2)), k2[1536:2304, :])
            cots = jnp.concatenate([cotr[e, 0, at(r, big), :], cotr[e, 1, at(r, big), :]], axis=1)
            delta = cots * slope(pre)
            low = delta.astype(BF16)
            d2[e, at(r, big, wide), 0:256] = low
            d2[e, at(r, big, wide), 256:384] = from_right(delta[:, 0:128], wide).astype(BF16)
            d2[e, at(r, big, wide), 384:512] = from_left(delta[:, 128:256], wide).astype(BF16)
            rounded = low.astype(F32)
            gb2s[...] += col_sum(rounded)
            pre2[e, at(r, big), :] = rounded

        loop(rows2 // big, body)
        d2t[:, e * rows2 : (e + 1) * rows2] = pre2[e].T.astype(BF16)

    for e in range(slab2):

        def body(r, e=e):
            out = dot_t(taps(d2, [e], r, big, (2, 1, 0)), g2[...])
            for k in range(3):
                part = out[:, k * 128 : (k + 1) * 128]
                first = k == 2 or e == 0
                gp[e + k, at(r, big), :] = part if first else gp[e + k, at(r, big), :] + part

        loop(rows2 // big, body)

    gps[0] = gp[0].astype(BF16)
    gps[1] = gp[slab2 + 1].astype(BF16)
    for c in range(2):
        send_halo(4 + c, *gp_halo(c))

    for k in range(3):
        for j in range(3):
            acc = None
            for e in range(slab2):
                one = dot(d2t[:, e * rows2 : (e + 1) * rows2], p2[e + k, j * wide : j * wide + rows2, :])
                acc = one if acc is None else acc + one
            t0, t1 = pltpu.roll(acc[0:128, 0:128], 64, 1), pltpu.roll(acc[0:128, 128:256], 64, 1)
            low = lanes(t0.shape) < 64
            f0 = jnp.where(low, t1, t0) + acc[128:256, 0:128]
            f1 = jnp.where(low, t0, t1) + acc[128:256, 128:256]
            base = (k * 3 + j) * 192
            s2x[base : base + 128, :] = f0.T.astype(BF16)
            s2x[base + 128 : base + 192, :] = f1.T[0:64, :].astype(BF16)
    bias = gb2s[...].sum(axis=0, keepdims=True)
    bias = bias[:, 0:128] + bias[:, 128:256]
    s2x[1728:1744, :] = jnp.broadcast_to(bias, (16, 128)).astype(BF16)
    if s2x.shape[0] > 1744:
        s2x[1744 : s2x.shape[0], :] = jnp.zeros((s2x.shape[0] - 1744, 128), BF16)

    sum2 = Sum(n, m, me, my, each2, s2x, s2got, s2part, s2gots, s2out, s2acc, (dsend2, drecv2, zsend2, zrecv2))
    sum1 = ShortSum(n, m, me, my, each1, s1x, s1got, s1part, s1gots, s1out, s1acc, (dsend1, drecv1, zsend1, zrecv1))
    sum2.step1()

    for c in range(2):
        wait_halo(4 + c, *gp_halo(c))
        for e in range(slab2):

            def body(r, e=e, c=c):
                r = r + c * (rows // 2 // small)
                total = gp[e + 1, at(r, small // 2), :]
                if e == 0:
                    total = total + gpr[0, at(r, small // 2), :].astype(F32)
                if e == slab2 - 1:
                    total = total + gpr[1, at(r, small // 2), :].astype(F32)
                total = total * 0.125
                turned = pltpu.roll(total, 64, 1)
                low = lanes(total.shape) < 64
                both = jnp.concatenate([jnp.where(low, total, turned), jnp.where(low, turned, total)], axis=1)
                both = both.reshape(small // 2 // wide, 1, wide, 256)
                both = jnp.broadcast_to(both, (small // 2 // wide, 2, wide, 256)).reshape(small, 256)
                for d in (2 * e, 2 * e + 1):
                    delta = both * slope(pre1[d, at(r, small), :])
                    low_delta = delta.astype(BF16)
                    d1[d, at(r, small, wide), 0:256] = low_delta
                    edge = jnp.where(
                        lanes((small, 128)) < 64,
                        from_right(delta[:, 0:128], wide),
                        from_left(delta[:, 128:256], wide),
                    )
                    d1[d, at(r, small, wide), 256:384] = edge.astype(BF16)
                    rounded = low_delta.astype(F32)
                    gb1s[...] += col_sum(rounded)
                    pre1[d, at(r, small), :] = rounded

            loop(rows // 2 // small, body)
    for d in range(slab):
        d1t[:, d * rows : (d + 1) * rows] = pre1[d].T.astype(BF16)

    for d in range(slab):

        def body(r, d=d):
            out = dot_t(taps(d1, [d], r, big, (2, 1, 0)), g1[...])
            for k in range(3):
                part = out[:, k * 128 : (k + 1) * 128]
                first = k == 2 or d == 0
                gx[d + k, at(r, big), :] = part if first else gx[d + k, at(r, big), :] + part

        loop(rows // big, body)
        if d == 0:
            gxs[0] = gx[0].astype(BF16)
    gxs[1] = gx[slab + 1].astype(BF16)
    sum2.step2()

    for k in range(3):
        for j in range(3):
            acc = None
            for d in range(slab):
                one = dot(d1t[:, d * rows : (d + 1) * rows], x2[d + k, j * wide : j * wide + rows, :])
                acc = one if acc is None else acc + one
            low = lanes((64, 128))
            total = acc[64:128, 0:128]
            total = total + jnp.where(
                low < 32, pltpu.roll(acc[0:64, 128:256], 32, 1), pltpu.roll(acc[0:64, 0:128], 32, 1)
            )
            total = total + pltpu.roll(acc[128:192, 0:128], 96, 1)
            total = total + jnp.where(
                low < 64, pltpu.roll(acc[192:256, 0:128], 64, 1), pltpu.roll(acc[192:256, 128:256], 64, 1)
            )
            t = k * 3 + j
            fold1[t % 5, (t // 5) * 64 : (t // 5) * 64 + 64, :] = total
    fold1[4, 64:128, :] = jnp.zeros((64, 128), F32)
    for t in range(5):
        s1x[t * 96 : t * 96 + 96, :] = fold1[t].T[0:96, :].astype(BF16)
    bias = gb1s[...].sum(axis=0, keepdims=True)
    bias = bias[:, 0:128] + bias[:, 128:256]
    bias = bias + pltpu.roll(bias, 64, 1)
    s1x[480:496, :] = jnp.broadcast_to(bias, (16, 128)).astype(BF16)
    if s1x.shape[0] > 496:
        s1x[496 : s1x.shape[0], :] = jnp.zeros((s1x.shape[0] - 496, 128), BF16)
    sum1.step1()
    sum2.step3()
    send_halo(6, *gx_halo)
    sum2.step4()
    sum1.step2()
    sum1.step3()
    wait_halo(6, *gx_halo)
    for d in range(slab):
        total = gx[d + 1]
        if d == 0:
            total = total + gxr[0].astype(F32)
        if d == slab - 1:
            total = total + gxr[1].astype(F32)
        xr[...] = total
        for g in range(wide):
            gin[0, d, :, g * 128 : (g + 1) * 128] = xr[pl.ds(g, side, stride=wide), :].astype(BF16)
    sum2.step5()
    sum1.step5()


def unpack(scale_one, scale_two, gin, s1out, s2out, gin_out, gw1, gb1, gw2, gb2):
    gin_out[...] = gin[...]
    for t in range(9):
        gw2[t] = s2out[t * 192 : (t + 1) * 192, :].astype(F32) * scale_two
    gb2[...] = s2out[1728:1744, :].astype(F32)[0:1, :] * scale_two
    for t in range(9):
        block = s1out[(t % 5) * 96 : (t % 5) * 96 + 96, :].astype(F32) * scale_one
        gw1[t] = block[:, (t // 5) * 64 : (t // 5) * 64 + 64]
    gb1[...] = s1out[480:496, :].astype(F32)[0:1, 0:64] * scale_one


def local(n, m, act_in, weight_one, bias_one, weight_two, bias_two, cotangent):
    samples, slab, side, merged = act_in.shape
    chan_in, chan_mid = weight_one.shape[3:]
    chan_out = weight_two.shape[4]
    slab2, half = cotangent.shape[1:3]
    assert samples == 1 and (chan_in, chan_mid, chan_out) == (32, 64, 128)
    scale_one = 16.0 / math.sqrt(samples * n * slab * m * side * side)
    scale_two = 1.0 / math.sqrt(samples * n * slab2 * m * half * half)
    wide = merged // 128
    rows, rows2 = side * wide, half * wide
    each = [-(-count // (n * m * 16)) * 16 for count in (496, 1744)]
    vmem = pltpu.VMEM

    def sums(size, slots):
        return [
            vmem((n * m * size, 128), BF16),
            vmem((n, m * size, 128), BF16),
            vmem((m * size, 128), BF16),
            vmem((m, slots * size, 128), BF16),
            vmem((m * size, 128), F32),
        ]

    dma = pltpu.SemaphoreType.DMA
    spec = pl.BlockSpec(memory_space=pltpu.VMEM)
    sent = pl.pallas_call(
        functools.partial(kernel, n, m, each[0], each[1]),
        out_shape=[
            jax.ShapeDtypeStruct(act_in.shape, BF16),
            jax.ShapeDtypeStruct((n * m * each[0], 128), BF16),
            jax.ShapeDtypeStruct((n * m * each[1], 128), BF16),
        ],
        in_specs=[spec] * 6,
        out_specs=[spec] * 3,
        scratch_shapes=[
            vmem((rows, 128), F32),
            vmem((slab + 2, rows + 2 * wide, 256), BF16),
            vmem((slab, rows, 256), F32),
            vmem((slab2, rows2, 128), BF16),
            vmem((slab2 + 2, rows2 + 2 * wide, 256), BF16),
            vmem((slab2, rows2, 256), F32),
            vmem((slab2, 2, rows2, 128), F32),
            vmem((slab2, rows2 + 2 * wide, 512), BF16),
            vmem((256, slab2 * rows2), BF16),
            vmem((slab2 + 2, rows2, 128), F32),
            vmem((slab, rows + 2 * wide, 384), BF16),
            vmem((256, slab * rows), BF16),
            vmem((slab + 2, rows, 128), F32),
            vmem((9 * 256, 256), BF16),
            vmem((9 * 256, 256), BF16),
            vmem((384, 3 * 384), BF16),
            vmem((384, 3 * 512), BF16),
            vmem((8, 256), F32),
            vmem((8, 256), F32),
            vmem((8, 256), F32),
            vmem((8, 256), F32),
            vmem((5, 128, 128), F32),
            vmem((2, side, merged), BF16),
            vmem((2, rows2, 128), BF16),
            vmem((2, rows2, 128), BF16),
            vmem((2, rows2, 128), BF16),
            vmem((2, rows, 128), BF16),
            vmem((2, rows, 128), BF16),
            *sums(each[1], 1),
            *sums(each[0], m),
            dma((14,)),
            dma((14,)),
            dma((2 * n,)),
            dma((2 * n,)),
            dma((2 * m,)),
            dma((2 * m,)),
            dma((2 * n,)),
            dma((2 * n,)),
            dma((2 * m,)),
            dma((2 * m,)),
        ],
        compiler_params=pltpu.CompilerParams(
            collective_id=0, has_side_effects=True, vmem_limit_bytes=60 * 1024 * 1024
        ),
    )(
        act_in,
        weight_one.reshape(27, chan_in, chan_mid),
        bias_one.reshape(1, chan_mid),
        weight_two.reshape(27, chan_mid, chan_out),
        bias_two.reshape(1, chan_out),
        cotangent,
    )
    outs = pl.pallas_call(
        functools.partial(unpack, scale_one, scale_two),
        out_shape=[
            jax.ShapeDtypeStruct(act_in.shape, BF16),
            jax.ShapeDtypeStruct((9, 3 * chan_in, chan_mid), F32),
            jax.ShapeDtypeStruct((1, chan_mid), F32),
            jax.ShapeDtypeStruct((9, 3 * chan_mid, chan_out), F32),
            jax.ShapeDtypeStruct((1, chan_out), F32),
        ],
        in_specs=[spec] * 3,
        out_specs=[spec] * 5,
    )(*sent)
    return (
        outs[0],
        outs[1].reshape(weight_one.shape),
        outs[2].reshape(bias_one.shape),
        outs[3].reshape(weight_two.shape),
        outs[4].reshape(bias_two.shape),
    )


def solution(mesh):
    placed = (P("dp", "space", None, None), P(), P(), P(), P(), P("dp", "space", None, None))
    return jax.shard_map(
        functools.partial(local, mesh.shape["dp"], mesh.shape["space"]),
        mesh=mesh,
        in_specs=placed,
        out_specs=(P("dp", "space", None, None), P(), P(), P(), P()),
        check_vma=False,
    )
```
